512 devices in a mesh: expert: 128 (over z, y, core), layer: 4 (over x).
Axes of the slice: x: 4, y: 8, z: 8, core: 2. Of those that a mesh axis runs over, the one named last changes fastest.
Arguments:
- gradient: bfloat16 [512, 256, 1536], P(('layer', 'expert')), parts along dimension 0, may hold values from -80 to 80
- prior_stat: float32 [512, 128], P('layer'), parts along dimension 0, may hold values from -600 to 600, as said below
Outputs:
- update: bfloat16 [512, 256, 1536], P(('layer', 'expert')), parts along dimension 0
- statistic: float32 [512, 128], P('layer'), parts along dimension 0
The draws below stay inside these ranges and needn't reach their ends.
There are 4 independent parts, one for each index of `layer`. The reference program is written for one: setup_inputs(seed, part) draws one part's arguments, and reference() takes and returns one part's arrays. A program takes and returns all parts, laid end to end along the dimension named above; each array names one. Nothing has to cross between parts.
Inputs may be any that keep to these rules, and one draw needn't show every extreme that they name: `prior_stat`: symmetric positive definite.
All inputs are finite; a program needn't handle non-finite values.
Results may differ from the reference program's by a relative error of at most 0.001.
The reference program's roundings to bfloat16 on the way count: a program that leaves them out, or rounds other values in their place, can miss the bound.
Values may be sent and summed in bfloat16 or wider, within the bound.
No kernel may reach another device: no remote copies, remote signals or barrier semaphores. Data moves between devices by JAX's collectives and lax.ppermute only.
A program may use at most 64 MiB of HBM per device.

```python
import jax
import jax.numpy as jnp
from jax import lax

F = 1536
ITERS = 5
EXPERTS = 128
D_SLAB = 256


def log_uniform(key, shape, low, high):
    return jnp.exp(jax.random.uniform(key, shape, jnp.float32, jnp.log(low), jnp.log(high)))


def draw_gradient(key, part):
    keys = jax.random.split(jax.random.fold_in(key, 11), 6)
    positions = jnp.arange(D_SLAB, dtype=jnp.float32) / max(D_SLAB - 1, 1)
    depth = 3.0 ** positions * log_uniform(keys[0], (D_SLAB,), 1.0, 2.0)
    column = log_uniform(keys[1], (F,), 0.3, 3.0)
    shared = jnp.clip(jax.random.normal(keys[2], (D_SLAB, F), jnp.float32), -4.0, 4.0)
    expert_scale = log_uniform(keys[3], (EXPERTS,), 0.56, 1.78)
    weight = jax.random.uniform(keys[4], (EXPERTS,), jnp.float32, -0.5, 0.5)
    noise = jnp.clip(jax.random.normal(keys[5], (EXPERTS, D_SLAB, F), jnp.float32), -4.0, 4.0)
    values = noise + weight[:, None, None] * shared[None]
    values = 0.25 * expert_scale[:, None, None] * depth[None, :, None] * column[None, None, :] * values
    return values.astype(jnp.bfloat16)


def draw_prior_stat(key, part):
    keys = jax.random.split(jax.random.fold_in(key, 23), 4)
    columns = 4 * EXPERTS
    scales = log_uniform(keys[0], (EXPERTS,), 0.56, 1.78)
    weight = jax.random.uniform(keys[1], (EXPERTS,), jnp.float32, -0.5, 0.5)
    noise = jnp.clip(jax.random.normal(keys[2], (EXPERTS, columns), jnp.float32), -4.0, 4.0)
    shared = jnp.clip(jax.random.normal(keys[3], (columns,), jnp.float32), -4.0, 4.0)
    basis = scales[:, None] * (noise + weight[:, None] * shared[None, :])
    product = jnp.dot(basis, basis.T, precision=lax.Precision.HIGHEST) / columns
    return product + 0.1 * jnp.diag(scales * scales)


def setup_inputs(seed: int = 0, part: int = 0) -> dict:
    splits = jax.random.split(jax.random.key(seed), 3)
    part_keys = jax.random.split(jax.random.fold_in(splits[2], part), 3)
    return {
        "gradient": draw_gradient(jax.random.fold_in(jax.random.fold_in(splits[2], part), 71), part),
        "prior_stat": draw_prior_stat(jax.random.fold_in(jax.random.fold_in(splits[2], part), 71), part),
    }


ridge_rate = 0.001
energy_floor = 1e-06

def matmul_high(left, right):
    return jnp.dot(left, right, precision=lax.Precision.HIGHEST, preferred_element_type=jnp.float32)

def inverse_root(statistic):
    count_rows = statistic.shape[0]
    identity = jnp.eye(count_rows, dtype=jnp.float32)
    ridge_term = ridge_rate * jnp.trace(statistic) / count_rows
    shifted = statistic + ridge_term * identity
    start_scale = 2.5 / jnp.sqrt(jnp.sum(shifted * shifted))
    matrix = start_scale * shifted
    root = start_scale ** 0.25 * identity
    for repeat in range(ITERS):
        factor = 1.25 * identity - 0.25 * matrix
        root = matmul_high(root, factor)
        square = matmul_high(factor, factor)
        matrix = matmul_high(matmul_high(square, square), matrix)
    return root

def reference(gradient, prior_stat):
    experts = gradient.shape[0]
    flattened = gradient.reshape(experts, -1)
    entries = flattened.shape[1]
    raw_gram = jnp.dot(flattened, flattened.T, preferred_element_type=jnp.float32)
    gram_mean = raw_gram / entries
    statistic = prior_stat + gram_mean
    root_bf = inverse_root(statistic).astype(jnp.bfloat16)
    products = jnp.dot(root_bf, flattened, preferred_element_type=jnp.float32)
    mixed_bf = products.astype(jnp.bfloat16)
    update_energy = jnp.sum(products * products) / (experts * entries)
    grad_energy = jnp.trace(gram_mean) / experts
    graft = jnp.sqrt((grad_energy + energy_floor) / (update_energy + energy_floor))
    fenced = lax.optimization_barrier(mixed_bf)
    update = (graft * fenced.astype(jnp.float32)).astype(jnp.bfloat16)
    return (update.reshape(gradient.shape), statistic)
```

```python
import jax
import jax.numpy as jnp
from jax import lax
from jax.experimental import pallas as pl
from jax.experimental.pallas import tpu as pltpu
from jax.sharding import Mesh
from jax.sharding import PartitionSpec as P

ITERS = 5
AXES = ("z4", "z2", "z1", "y4", "y2", "y1", "core")
LAYER_EXPERT = ("layer",) + AXES
NEAR = ("z1", "y1", "core")
FAR = ("z4", "z2", "y4", "y2")

ridge_rate = 0.001
energy_floor = 1e-06

VMEM = pl.BlockSpec(memory_space=pltpu.VMEM)


def matmul_high(left, right):
    return jnp.dot(left, right, precision=lax.Precision.HIGHEST, preferred_element_type=jnp.float32)


def peers_of(axes):
    peers = 1
    for axis in axes:
        peers *= lax.axis_size(axis)
    return peers


def exchanged(pieces, axes):
    return lax.all_to_all(pieces, axes, split_axis=0, concat_axis=0, tiled=True)


def from_everyone(shard, axes):
    return exchanged(jnp.broadcast_to(shard[None], (peers_of(axes), *shard.shape)), axes)


def summed_over_all(gram):
    rows, width = gram.shape
    near = peers_of(NEAR)
    own = jnp.sum(exchanged(gram.reshape(near, rows // near, width), NEAR), axis=0)
    own = jnp.sum(from_everyone(own, FAR), axis=0)
    return from_everyone(own, NEAR).reshape(rows, width)


def whole_sum(array):
    return jnp.sum(jnp.sum(array, axis=0, keepdims=True), axis=1, keepdims=True)


def root_and_products(entry_count, gram_sum, prior_stat, flattened):
    experts = prior_stat.shape[0]
    rows = 8
    width = flattened.shape[1] // rows
    lanes = 128
    tiles = width // lanes

    def kernel(gram_ref, prior_ref, flat_ref, stat_ref, root_ref, mixed_ref, wide_ref):
        shape = (experts, experts)
        diagonal = lax.broadcasted_iota(jnp.int32, shape, 0) == lax.broadcasted_iota(jnp.int32, shape, 1)
        statistic = prior_ref[...] + gram_ref[...] * (1.0 / entry_count)
        stat_ref[...] = statistic
        ridge = whole_sum(jnp.where(diagonal, statistic, 0.0)) * (ridge_rate / experts)
        shifted = statistic + jnp.where(diagonal, ridge, 0.0)
        start = 2.5 / jnp.sqrt(whole_sum(shifted * shifted))
        scaled_identity = jnp.where(diagonal, 1.25, 0.0)
        matrix = start * shifted
        factor = scaled_identity - 0.25 * matrix
        root = jnp.sqrt(jnp.sqrt(start)) * factor
        for repeat in range(ITERS - 1):
            square = matmul_high(factor, factor)
            matrix = matmul_high(matmul_high(square, square), matrix)
            factor = scaled_identity - 0.25 * matrix
            root = matmul_high(root, factor)
        root_bf = root.astype(jnp.bfloat16)
        root_ref[...] = root_bf
        for row in range(rows):
            part = jnp.dot(root_bf, flat_ref[:, row * width : (row + 1) * width], preferred_element_type=jnp.float32)
            for tile in range(tiles):
                wide_ref[tile, pl.ds(row, experts, stride=rows), :] = part[:, tile * lanes : (tile + 1) * lanes]
        for tile in range(tiles):
            mixed_ref[:, :, tile * lanes : (tile + 1) * lanes] = (
                wide_ref[tile].reshape(experts, rows, lanes).astype(jnp.bfloat16)
            )

    return pl.pallas_call(
        kernel,
        out_shape=(
            jax.ShapeDtypeStruct((experts, experts), jnp.float32),
            jax.ShapeDtypeStruct((experts, experts), jnp.bfloat16),
            jax.ShapeDtypeStruct((experts, rows, width), jnp.bfloat16),
        ),
        in_specs=[VMEM] * 3,
        out_specs=(VMEM,) * 3,
        scratch_shapes=[pltpu.VMEM((tiles, experts * rows, lanes), jnp.float32)],
        name="root_and_products",
    )(gram_sum, prior_stat, flattened)


def body(gradient, prior_stat):
    experts = prior_stat.shape[0]
    slab_rows, width = gradient.shape[1:]
    entry_count = slab_rows * width
    rows = 8
    blocks = slab_rows // rows
    columns = experts // blocks
    piece = width // columns
    pieces = gradient.reshape(blocks, rows, columns, piece).transpose(0, 2, 1, 3).reshape(experts, rows, piece)
    regrouped = exchanged(pieces, AXES)
    flattened = regrouped.reshape(experts, rows * piece)
    gram = jnp.einsum("ek,gk->eg", flattened, flattened, preferred_element_type=jnp.float32)
    gram_sum = summed_over_all(gram)
    statistic, root_bf, mixed_bf = root_and_products(entry_count, gram_sum, prior_stat, flattened)
    returned = exchanged(mixed_bf, AXES)
    gram_mean = gram_sum / entry_count
    root_wide = root_bf.astype(jnp.float32)
    update_energy = jnp.sum(matmul_high(root_wide, gram_mean) * root_wide) / experts
    grad_energy = jnp.trace(gram_mean) / experts
    graft = jnp.sqrt((grad_energy + energy_floor) / (update_energy + energy_floor))
    update = (graft * returned.astype(jnp.float32)).astype(jnp.bfloat16)
    update = update.reshape(blocks, columns, rows, piece).transpose(0, 2, 1, 3).reshape(gradient.shape)
    return (update, statistic)


def solution(mesh):
    torus = Mesh(
        mesh.devices.reshape(2, 2, 2, 2, 2, 2, 2, mesh.shape["layer"]),
        AXES + ("layer",),
    )
    return jax.shard_map(
        body,
        mesh=torus,
        in_specs=(P(LAYER_EXPERT, None, None), P("layer", None)),
        out_specs=(P(LAYER_EXPERT, None, None), P("layer", None)),
        check_vma=False,
    )
```

```python
import jax
import jax.numpy as jnp
from jax import lax
from jax.experimental import pallas as pl
from jax.experimental.pallas import tpu as pltpu
from jax.sharding import Mesh
from jax.sharding import PartitionSpec as P

ITERS = 5
AXES = ("z4", "z2", "z1", "y4", "y2", "y1", "core")
LAYER_EXPERT = ("layer",) + AXES
NEAR = ("z1", "y1", "core")
FAR = ("z4", "z2", "y4", "y2")

ridge_rate = 0.001
energy_floor = 1e-06

ROWS = 8
LANES = 128

VMEM = pl.BlockSpec(memory_space=pltpu.VMEM)


def matmul_high(left, right):
    return jnp.dot(left, right, precision=lax.Precision.HIGHEST, preferred_element_type=jnp.float32)


def peers_of(axes):
    peers = 1
    for axis in axes:
        peers *= lax.axis_size(axis)
    return peers


def exchanged(pieces, axes):
    return lax.all_to_all(pieces, axes, split_axis=0, concat_axis=0, tiled=True)


def from_everyone(shard, axes):
    return exchanged(jnp.broadcast_to(shard[None], (peers_of(axes), *shard.shape)), axes)


def summed_over_all(gram):
    rows, width = gram.shape
    near = peers_of(NEAR)
    own = jnp.sum(exchanged(gram.reshape(near, rows // near, width), NEAR), axis=0)
    own = jnp.sum(from_everyone(own, FAR), axis=0)
    return from_everyone(own, NEAR).reshape(rows, width)


def in_vmem(array):
    return pltpu.with_memory_space_constraint(array, pltpu.VMEM)


def whole_sum(array):
    return jnp.sum(jnp.sum(array, axis=0, keepdims=True), axis=1, keepdims=True)


def widen_rows(pieces_ref, wide_ref):
    for tile in range(wide_ref.shape[0]):
        lanes = pieces_ref[:, :, tile * LANES : (tile + 1) * LANES]
        wide_ref[tile] = lanes.astype(jnp.float32).reshape(wide_ref.shape[1:])


def one_row(wide_ref, row, experts, rows):
    parts = [wide_ref[tile, pl.ds(row, experts, stride=rows), :] for tile in range(wide_ref.shape[0])]
    return jnp.concatenate(parts, axis=1).astype(jnp.bfloat16)


def wide_scratch(experts, rows, width):
    return pltpu.VMEM((width // LANES, experts * rows, LANES), jnp.float32)


def piece_gram(pieces):
    experts, rows, width = pieces.shape

    def kernel(pieces_ref, gram_ref, wide_ref):
        widen_rows(pieces_ref, wide_ref)
        gram = jnp.zeros((experts, experts), jnp.float32)
        for row in range(rows):
            line = one_row(wide_ref, row, experts, rows)
            gram += lax.dot_general(line, line, (((1,), (1,)), ((), ())), preferred_element_type=jnp.float32)
        gram_ref[...] = gram

    return pl.pallas_call(
        kernel,
        out_shape=pltpu.VMEM((experts, experts), jnp.float32),
        in_specs=[VMEM],
        out_specs=VMEM,
        scratch_shapes=[wide_scratch(experts, rows, width)],
        name="piece_gram",
    )(in_vmem(pieces))


def grafted_products(entry_count, gram_sum, prior_stat, pieces):
    experts, rows, width = pieces.shape

    def kernel(gram_ref, prior_ref, pieces_ref, stat_ref, update_ref, wide_ref, out_ref):
        widen_rows(pieces_ref, wide_ref)
        shape = (experts, experts)
        diagonal = lax.broadcasted_iota(jnp.int32, shape, 0) == lax.broadcasted_iota(jnp.int32, shape, 1)
        gram_mean = gram_ref[...] * (1.0 / entry_count)
        statistic = prior_ref[...] + gram_mean
        stat_ref[...] = statistic
        ridge = whole_sum(jnp.where(diagonal, statistic, 0.0)) * (ridge_rate / experts)
        shifted = statistic + jnp.where(diagonal, ridge, 0.0)
        start = 2.5 / jnp.sqrt(whole_sum(shifted * shifted))
        scaled_identity = jnp.where(diagonal, 1.25, 0.0)
        matrix = start * shifted
        factor = scaled_identity - 0.25 * matrix
        root = jnp.sqrt(jnp.sqrt(start)) * factor
        for repeat in range(ITERS - 1):
            square = matmul_high(factor, factor)
            matrix = matmul_high(matmul_high(square, square), matrix)
            factor = scaled_identity - 0.25 * matrix
            root = matmul_high(root, factor)
        root_bf = root.astype(jnp.bfloat16)
        root_wide = root_bf.astype(jnp.float32)
        update_energy = whole_sum(matmul_high(root_wide, gram_mean) * root_wide) / experts
        grad_energy = whole_sum(jnp.where(diagonal, gram_mean, 0.0)) / experts
        graft = jnp.sqrt((grad_energy + energy_floor) / (update_energy + energy_floor))
        for row in range(rows):
            line = one_row(wide_ref, row, experts, rows)
            mixed_bf = jnp.dot(root_bf, line, preferred_element_type=jnp.float32).astype(jnp.bfloat16)
            update = graft * mixed_bf.astype(jnp.float32)
            for tile in range(width // LANES):
                out_ref[tile, pl.ds(row, experts, stride=rows), :] = update[:, tile * LANES : (tile + 1) * LANES]
        for tile in range(width // LANES):
            update_ref[:, :, tile * LANES : (tile + 1) * LANES] = (
                out_ref[tile].reshape(experts, rows, LANES).astype(jnp.bfloat16)
            )

    return pl.pallas_call(
        kernel,
        out_shape=(
            pltpu.VMEM((experts, experts), jnp.float32),
            pltpu.VMEM(pieces.shape, jnp.bfloat16),
        ),
        in_specs=[VMEM] * 3,
        out_specs=(VMEM,) * 2,
        scratch_shapes=[wide_scratch(experts, rows, width)] * 2,
        name="grafted_products",
    )(in_vmem(gram_sum), in_vmem(prior_stat), in_vmem(pieces))


def body(gradient, prior_stat):
    experts = prior_stat.shape[0]
    slab_rows, width = gradient.shape[1:]
    blocks = slab_rows // ROWS
    columns = experts // blocks
    piece = width // columns
    pieces = gradient.reshape(blocks, ROWS, columns, piece).transpose(0, 2, 1, 3).reshape(experts, ROWS, piece)
    regrouped = exchanged(pieces, AXES)
    gram_sum = summed_over_all(piece_gram(regrouped))
    statistic, scaled = grafted_products(slab_rows * width, gram_sum, prior_stat, regrouped)
    returned = exchanged(scaled, AXES)
    update = returned.reshape(blocks, columns, ROWS, piece).transpose(0, 2, 1, 3).reshape(gradient.shape)
    return (update, statistic)


def solution(mesh):
    torus = Mesh(
        mesh.devices.reshape(2, 2, 2, 2, 2, 2, 2, mesh.shape["layer"]),
        AXES + ("layer",),
    )
    return jax.shard_map(
        body,
        mesh=torus,
        in_specs=(P(LAYER_EXPERT, None, None), P("layer", None)),
        out_specs=(P(LAYER_EXPERT, None, None), P("layer", None)),
        check_vma=False,
    )
```

```python
import jax
import jax.numpy as jnp
from jax import lax
from jax.experimental import pallas as pl
from jax.experimental.pallas import tpu as pltpu
from jax.sharding import Mesh
from jax.sharding import PartitionSpec as P

ITERS = 5
AXES = ("z4", "z2", "z1", "y4", "y2", "y1", "core")
LAYER_EXPERT = ("layer",) + AXES
NEAR = ("z1", "y1", "core")
FAR = ("z4", "z2", "y4", "y2")

ridge_rate = 0.001
energy_floor = 1e-06

ROWS = 8
LANES = 128

VMEM = pl.BlockSpec(memory_space=pltpu.VMEM)


def matmul_high(left, right):
    return jnp.dot(left, right, precision=lax.Precision.HIGHEST, preferred_element_type=jnp.float32)


def peers_of(axes):
    peers = 1
    for axis in axes:
        peers *= lax.axis_size(axis)
    return peers


def exchanged(pieces, axes):
    return lax.all_to_all(pieces, axes, split_axis=0, concat_axis=0, tiled=True)


def from_everyone(shard, axes):
    return exchanged(jnp.broadcast_to(shard[None], (peers_of(axes), *shard.shape)), axes)


def summed_over_all(gram):
    rows, width = gram.shape
    near = peers_of(NEAR)
    own = jnp.sum(exchanged(gram.reshape(near, rows // near, width), NEAR), axis=0)
    own = jnp.sum(from_everyone(own, FAR), axis=0)
    return from_everyone(own, NEAR).reshape(rows, width)


def in_vmem(array):
    return pltpu.with_memory_space_constraint(array, pltpu.VMEM)


def whole_sum(array):
    return jnp.sum(jnp.sum(array, axis=0, keepdims=True), axis=1, keepdims=True)


def widen_rows(pieces_ref, wide_ref):
    for tile in range(wide_ref.shape[0]):
        lanes = pieces_ref[:, :, tile * LANES : (tile + 1) * LANES]
        wide_ref[tile] = lanes.astype(jnp.float32).reshape(wide_ref.shape[1:])


def one_row(wide_ref, row, experts, rows):
    parts = [wide_ref[tile, pl.ds(row, experts, stride=rows), :] for tile in range(wide_ref.shape[0])]
    return jnp.concatenate(parts, axis=1).astype(jnp.bfloat16)


def wide_scratch(experts, rows, width):
    return pltpu.VMEM((width // LANES, experts * rows, LANES), jnp.float32)


def piece_gram(pieces):
    experts, rows, width = pieces.shape

    def kernel(pieces_ref, gram_ref, wide_ref):
        widen_rows(pieces_ref, wide_ref)
        gram = jnp.zeros((experts, experts), jnp.float32)
        for row in range(rows):
            line = one_row(wide_ref, row, experts, rows)
            gram += lax.dot_general(line, line, (((1,), (1,)), ((), ())), preferred_element_type=jnp.float32)
        gram_ref[...] = gram

    return pl.pallas_call(
        kernel,
        out_shape=pltpu.VMEM((experts, experts), jnp.float32),
        in_specs=[VMEM],
        out_specs=VMEM,
        scratch_shapes=[wide_scratch(experts, rows, width)],
        name="piece_gram",
    )(in_vmem(pieces))


def grafted_products(entry_count, gram_sum, prior_stat, pieces):
    experts, rows, width = pieces.shape

    def kernel(gram_ref, prior_ref, pieces_ref, stat_ref, update_ref, wide_ref, out_ref, held_ref, arrival):
        widen_rows(pieces_ref, wide_ref)
        shape = (experts, experts)
        diagonal = lax.broadcasted_iota(jnp.int32, shape, 0) == lax.broadcasted_iota(jnp.int32, shape, 1)
        gram_mean = gram_ref[...] * (1.0 / entry_count)
        statistic = prior_ref[...] + gram_mean
        held_ref[...] = statistic
        written = pltpu.make_async_copy(held_ref, stat_ref, arrival)
        written.start()
        ridge = whole_sum(jnp.where(diagonal, statistic, 0.0)) * (ridge_rate / experts)
        shifted = statistic + jnp.where(diagonal, ridge, 0.0)
        start = 2.5 / jnp.sqrt(whole_sum(shifted * shifted))
        scaled_identity = jnp.where(diagonal, 1.25, 0.0)
        matrix = start * shifted
        factor = scaled_identity - 0.25 * matrix
        root = jnp.sqrt(jnp.sqrt(start)) * factor
        for repeat in range(ITERS - 1):
            square = matmul_high(factor, factor)
            matrix = matmul_high(matmul_high(square, square), matrix)
            factor = scaled_identity - 0.25 * matrix
            root = matmul_high(root, factor)
        root_bf = root.astype(jnp.bfloat16)
        root_wide = root_bf.astype(jnp.float32)
        update_energy = whole_sum(matmul_high(root_wide, gram_mean) * root_wide) / experts
        grad_energy = whole_sum(jnp.where(diagonal, gram_mean, 0.0)) / experts
        graft = jnp.sqrt((grad_energy + energy_floor) / (update_energy + energy_floor))
        for row in range(rows):
            line = one_row(wide_ref, row, experts, rows)
            mixed_bf = jnp.dot(root_bf, line, preferred_element_type=jnp.float32).astype(jnp.bfloat16)
            update = graft * mixed_bf.astype(jnp.float32)
            for tile in range(width // LANES):
                out_ref[tile, pl.ds(row, experts, stride=rows), :] = update[:, tile * LANES : (tile + 1) * LANES]
        for tile in range(width // LANES):
            update_ref[:, :, tile * LANES : (tile + 1) * LANES] = (
                out_ref[tile].reshape(experts, rows, LANES).astype(jnp.bfloat16)
            )
        written.wait()

    return pl.pallas_call(
        kernel,
        out_shape=(
            pltpu.HBM((experts, experts), jnp.float32),
            pltpu.VMEM(pieces.shape, jnp.bfloat16),
        ),
        in_specs=[VMEM] * 3,
        out_specs=(pl.BlockSpec(memory_space=pltpu.HBM), VMEM),
        scratch_shapes=[
            wide_scratch(experts, rows, width),
            wide_scratch(experts, rows, width),
            pltpu.VMEM((experts, experts), jnp.float32),
            pltpu.SemaphoreType.DMA,
        ],
        name="grafted_products",
    )(in_vmem(gram_sum), in_vmem(prior_stat), in_vmem(pieces))


def body(gradient, prior_stat):
    experts = prior_stat.shape[0]
    slab_rows, width = gradient.shape[1:]
    blocks = slab_rows // ROWS
    columns = experts // blocks
    piece = width // columns
    pieces = gradient.reshape(blocks, ROWS, columns, piece).transpose(0, 2, 1, 3).reshape(experts, ROWS, piece)
    regrouped = exchanged(pieces, AXES)
    gram_sum = summed_over_all(piece_gram(regrouped))
    statistic, scaled = grafted_products(slab_rows * width, gram_sum, prior_stat, regrouped)
    returned = exchanged(scaled, AXES)
    update = returned.reshape(blocks, columns, ROWS, piece).transpose(0, 2, 1, 3).reshape(gradient.shape)
    return (update, statistic)


def solution(mesh):
    torus = Mesh(
        mesh.devices.reshape(2, 2, 2, 2, 2, 2, 2, mesh.shape["layer"]),
        AXES + ("layer",),
    )
    return jax.shard_map(
        body,
        mesh=torus,
        in_specs=(P(LAYER_EXPERT, None, None), P("layer", None)),
        out_specs=(P(LAYER_EXPERT, None, None), P("layer", None)),
        check_vma=False,
    )
```

```python
import jax
import jax.numpy as jnp
from jax import lax
from jax.experimental import pallas as pl
from jax.experimental.pallas import tpu as pltpu
from jax.sharding import Mesh
from jax.sharding import PartitionSpec as P

ITERS = 5
AXES = ("z4", "z2", "z1", "y4", "y2", "y1", "core")
LAYER_EXPERT = ("layer",) + AXES
NEAR = ("z1", "y1", "core")
FAR = ("z4", "z2", "y4", "y2")

ridge_rate = 0.001
energy_floor = 1e-06

ROWS = 8
LANES = 128

VMEM = pl.BlockSpec(memory_space=pltpu.VMEM)


def matmul_high(left, right):
    return jnp.dot(left, right, precision=lax.Precision.HIGHEST, preferred_element_type=jnp.float32)


def split_three(wide):
    high = wide.astype(jnp.bfloat16)
    rest = wide - high.astype(jnp.float32)
    middle = rest.astype(jnp.bfloat16)
    return high, middle, (rest - middle.astype(jnp.float32)).astype(jnp.bfloat16)


def peers_of(axes):
    peers = 1
    for axis in axes:
        peers *= lax.axis_size(axis)
    return peers


def exchanged(pieces, axes):
    return lax.all_to_all(pieces, axes, split_axis=0, concat_axis=0, tiled=True)


def from_everyone(shard, axes):
    return exchanged(jnp.broadcast_to(shard[None], (peers_of(axes), *shard.shape)), axes)


def summed_over_all(gram):
    rows, width = gram.shape
    near = peers_of(NEAR)
    own = jnp.sum(exchanged(gram.reshape(near, rows // near, width), NEAR), axis=0)
    own = jnp.sum(from_everyone(own, FAR), axis=0)
    return from_everyone(own, NEAR).reshape(rows, width)


def in_vmem(array):
    return pltpu.with_memory_space_constraint(array, pltpu.VMEM)


def whole_sum(array):
    return jnp.sum(jnp.sum(array, axis=0, keepdims=True), axis=1, keepdims=True)


def widen_rows(pieces_ref, wide_ref):
    for tile in range(wide_ref.shape[0]):
        lanes = pieces_ref[:, :, tile * LANES : (tile + 1) * LANES]
        wide_ref[tile] = lanes.astype(jnp.float32).reshape(wide_ref.shape[1:])


def one_row(wide_ref, row, experts, rows):
    parts = [wide_ref[tile, pl.ds(row, experts, stride=rows), :] for tile in range(wide_ref.shape[0])]
    return jnp.concatenate(parts, axis=1).astype(jnp.bfloat16)


def wide_scratch(experts, rows, width):
    return pltpu.VMEM((width // LANES, experts * rows, LANES), jnp.float32)


def piece_gram(pieces):
    experts, rows, width = pieces.shape

    def kernel(pieces_ref, gram_ref, wide_ref):
        widen_rows(pieces_ref, wide_ref)
        gram = jnp.zeros((experts, experts), jnp.float32)
        for row in range(rows):
            line = one_row(wide_ref, row, experts, rows)
            gram += lax.dot_general(line, line, (((1,), (1,)), ((), ())), preferred_element_type=jnp.float32)
        gram_ref[...] = gram

    return pl.pallas_call(
        kernel,
        out_shape=pltpu.VMEM((experts, experts), jnp.float32),
        in_specs=[VMEM],
        out_specs=VMEM,
        scratch_shapes=[wide_scratch(experts, rows, width)],
        name="piece_gram",
    )(in_vmem(pieces))


def grafted_products(entry_count, gram_sum, prior_stat, pieces):
    experts, rows, width = pieces.shape

    def kernel(gram_ref, prior_ref, pieces_ref, stat_ref, update_ref, wide_ref, out_ref, held_ref, arrival):
        widen_rows(pieces_ref, wide_ref)
        shape = (experts, experts)
        diagonal = lax.broadcasted_iota(jnp.int32, shape, 0) == lax.broadcasted_iota(jnp.int32, shape, 1)
        gram_mean = gram_ref[...] * (1.0 / entry_count)
        statistic = prior_ref[...] + gram_mean
        held_ref[...] = statistic
        written = pltpu.make_async_copy(held_ref, stat_ref, arrival)
        ridge = whole_sum(jnp.where(diagonal, statistic, 0.0)) * (ridge_rate / experts)
        shifted = statistic + jnp.where(diagonal, ridge, 0.0)
        start = 2.5 * lax.rsqrt(whole_sum(shifted * shifted))
        scaled_identity = jnp.where(diagonal, 1.25, 0.0)
        matrix = start * shifted
        factor = scaled_identity - 0.25 * matrix
        root = jnp.sqrt(jnp.sqrt(start)) * factor
        for repeat in range(ITERS - 1):
            square = matmul_high(factor, factor)
            matrix = matmul_high(matmul_high(square, square), matrix)
            factor = scaled_identity - 0.25 * matrix
            root = matmul_high(root, factor)
            if repeat == 0:
                written.start()
        root_bf = root.astype(jnp.bfloat16)
        root_gram = jnp.dot(
            jnp.concatenate([root_bf] * 3, axis=1),
            jnp.concatenate(split_three(gram_mean), axis=0),
            preferred_element_type=jnp.float32,
        )
        update_energy = whole_sum(root_gram * root_bf.astype(jnp.float32)) / experts
        grad_energy = whole_sum(jnp.where(diagonal, gram_mean, 0.0)) / experts
        graft = jnp.sqrt((grad_energy + energy_floor) / (update_energy + energy_floor))
        for row in range(rows):
            line = one_row(wide_ref, row, experts, rows)
            mixed_bf = jnp.dot(root_bf, line, preferred_element_type=jnp.float32).astype(jnp.bfloat16)
            update = graft * mixed_bf.astype(jnp.float32)
            for tile in range(width // LANES):
                out_ref[tile, pl.ds(row, experts, stride=rows), :] = update[:, tile * LANES : (tile + 1) * LANES]
        for tile in range(width // LANES):
            update_ref[:, :, tile * LANES : (tile + 1) * LANES] = (
                out_ref[tile].reshape(experts, rows, LANES).astype(jnp.bfloat16)
            )
        written.wait()

    return pl.pallas_call(
        kernel,
        out_shape=(
            pltpu.HBM((experts, experts), jnp.float32),
            pltpu.VMEM(pieces.shape, jnp.bfloat16),
        ),
        in_specs=[VMEM] * 3,
        out_specs=(pl.BlockSpec(memory_space=pltpu.HBM), VMEM),
        scratch_shapes=[
            wide_scratch(experts, rows, width),
            wide_scratch(experts, rows, width),
            pltpu.VMEM((experts, experts), jnp.float32),
            pltpu.SemaphoreType.DMA,
        ],
        name="grafted_products",
    )(in_vmem(gram_sum), in_vmem(prior_stat), in_vmem(pieces))


def body(gradient, prior_stat):
    experts = prior_stat.shape[0]
    slab_rows, width = gradient.shape[1:]
    blocks = slab_rows // ROWS
    columns = experts // blocks
    piece = width // columns
    pieces = gradient.reshape(blocks, ROWS, columns, piece).transpose(0, 2, 1, 3).reshape(experts, ROWS, piece)
    regrouped = exchanged(pieces, AXES)
    gram_sum = summed_over_all(piece_gram(regrouped))
    statistic, scaled = grafted_products(slab_rows * width, gram_sum, prior_stat, regrouped)
    returned = exchanged(scaled, AXES)
    update = returned.reshape(blocks, columns, ROWS, piece).transpose(0, 2, 1, 3).reshape(gradient.shape)
    return (update, statistic)


def solution(mesh):
    torus = Mesh(
        mesh.devices.reshape(2, 2, 2, 2, 2, 2, 2, mesh.shape["layer"]),
        AXES + ("layer",),
    )
    return jax.shard_map(
        body,
        mesh=torus,
        in_specs=(P(LAYER_EXPERT, None, None), P("layer", None)),
        out_specs=(P(LAYER_EXPERT, None, None), P("layer", None)),
        check_vma=False,
    )
```

```python
import jax
import jax.numpy as jnp
from jax import lax
from jax.experimental import pallas as pl
from jax.experimental.pallas import tpu as pltpu
from jax.sharding import Mesh
from jax.sharding import PartitionSpec as P

ITERS = 5
AXES = ("z4", "z2", "z1", "y4", "y2", "y1", "core")
LAYER_EXPERT = ("layer",) + AXES
NEAR = ("z1", "y1", "core")
FAR = ("z4", "z2", "y4", "y2")

ridge_rate = 0.001
energy_floor = 1e-06

ROWS = 8
LANES = 128

VMEM = pl.BlockSpec(memory_space=pltpu.VMEM)


def matmul_high(left, right):
    return jnp.dot(left, right, precision=lax.Precision.HIGHEST, preferred_element_type=jnp.float32)


def split_three(wide):
    high = wide.astype(jnp.bfloat16)
    rest = wide - high.astype(jnp.float32)
    middle = rest.astype(jnp.bfloat16)
    return high, middle, (rest - middle.astype(jnp.float32)).astype(jnp.bfloat16)


def peers_of(axes):
    peers = 1
    for axis in axes:
        peers *= lax.axis_size(axis)
    return peers


def exchanged(pieces, axes):
    return lax.all_to_all(pieces, axes, split_axis=0, concat_axis=0, tiled=True)


def from_everyone(shard, axes):
    return exchanged(jnp.broadcast_to(shard[None], (peers_of(axes), *shard.shape)), axes)


def summed_over_all(gram):
    rows, width = gram.shape
    near = peers_of(NEAR)
    own = jnp.sum(exchanged(gram.reshape(near, rows // near, width), NEAR), axis=0)
    own = jnp.sum(from_everyone(own, FAR), axis=0)
    return from_everyone(own, NEAR).reshape(rows, width)


def in_vmem(array):
    return pltpu.with_memory_space_constraint(array, pltpu.VMEM)


def whole_sum(array):
    return jnp.sum(jnp.sum(array, axis=0, keepdims=True), axis=1, keepdims=True)


def widen_rows(pieces_ref, wide_ref):
    for tile in range(wide_ref.shape[0]):
        lanes = pieces_ref[:, :, tile * LANES : (tile + 1) * LANES]
        wide_ref[tile] = lanes.astype(jnp.float32).reshape(wide_ref.shape[1:])


def one_row(wide_ref, row, experts, rows):
    parts = [wide_ref[tile, pl.ds(row, experts, stride=rows), :] for tile in range(wide_ref.shape[0])]
    return jnp.concatenate(parts, axis=1).astype(jnp.bfloat16)


def wide_scratch(experts, rows, width):
    return pltpu.VMEM((width // LANES, experts * rows, LANES), jnp.float32)


def piece_gram(pieces):
    experts, rows, width = pieces.shape

    def kernel(pieces_ref, gram_ref, lines_ref, wide_ref):
        widen_rows(pieces_ref, wide_ref)
        gram = jnp.zeros((experts, experts), jnp.float32)
        for row in range(rows):
            line = one_row(wide_ref, row, experts, rows)
            lines_ref[row] = line
            gram += lax.dot_general(line, line, (((1,), (1,)), ((), ())), preferred_element_type=jnp.float32)
        gram_ref[...] = gram

    return pl.pallas_call(
        kernel,
        out_shape=(
            pltpu.VMEM((experts, experts), jnp.float32),
            pltpu.VMEM((rows, experts, width), jnp.bfloat16),
        ),
        in_specs=[VMEM],
        out_specs=(VMEM,) * 2,
        scratch_shapes=[wide_scratch(experts, rows, width)],
        name="piece_gram",
    )(in_vmem(pieces))


def grafted_products(entry_count, gram_sum, prior_stat, lines):
    rows, experts, width = lines.shape

    def kernel(gram_ref, prior_ref, lines_ref, stat_ref, update_ref, out_ref, held_ref, arrival):
        shape = (experts, experts)
        diagonal = lax.broadcasted_iota(jnp.int32, shape, 0) == lax.broadcasted_iota(jnp.int32, shape, 1)
        gram_mean = gram_ref[...] * (1.0 / entry_count)
        statistic = prior_ref[...] + gram_mean
        held_ref[...] = statistic
        written = pltpu.make_async_copy(held_ref, stat_ref, arrival)
        ridge = whole_sum(jnp.where(diagonal, statistic, 0.0)) * (ridge_rate / experts)
        shifted = statistic + jnp.where(diagonal, ridge, 0.0)
        start = 2.5 * lax.rsqrt(whole_sum(shifted * shifted))
        scaled_identity = jnp.where(diagonal, 1.25, 0.0)
        matrix = start * shifted
        factor = scaled_identity - 0.25 * matrix
        root = jnp.sqrt(jnp.sqrt(start)) * factor
        for repeat in range(ITERS - 1):
            square = matmul_high(factor, factor)
            matrix = matmul_high(matmul_high(square, square), matrix)
            factor = scaled_identity - 0.25 * matrix
            root = matmul_high(root, factor)
            if repeat == 0:
                written.start()
        root_bf = root.astype(jnp.bfloat16)
        root_gram = jnp.dot(
            jnp.concatenate([root_bf] * 3, axis=1),
            jnp.concatenate(split_three(gram_mean), axis=0),
            preferred_element_type=jnp.float32,
        )
        update_energy = whole_sum(root_gram * root_bf.astype(jnp.float32)) / experts
        grad_energy = whole_sum(jnp.where(diagonal, gram_mean, 0.0)) / experts
        graft = jnp.sqrt((grad_energy + energy_floor) / (update_energy + energy_floor))
        for row in range(rows):
            mixed_bf = jnp.dot(root_bf, lines_ref[row], preferred_element_type=jnp.float32).astype(jnp.bfloat16)
            update = graft * mixed_bf.astype(jnp.float32)
            for tile in range(width // LANES):
                out_ref[tile, pl.ds(row, experts, stride=rows), :] = update[:, tile * LANES : (tile + 1) * LANES]
        for tile in range(width // LANES):
            update_ref[:, :, tile * LANES : (tile + 1) * LANES] = (
                out_ref[tile].reshape(experts, rows, LANES).astype(jnp.bfloat16)
            )
        written.wait()

    return pl.pallas_call(
        kernel,
        out_shape=(
            pltpu.HBM((experts, experts), jnp.float32),
            pltpu.VMEM((experts, rows, width), jnp.bfloat16),
        ),
        in_specs=[VMEM] * 3,
        out_specs=(pl.BlockSpec(memory_space=pltpu.HBM), VMEM),
        scratch_shapes=[
            wide_scratch(experts, rows, width),
            pltpu.VMEM((experts, experts), jnp.float32),
            pltpu.SemaphoreType.DMA,
        ],
        name="grafted_products",
    )(in_vmem(gram_sum), in_vmem(prior_stat), in_vmem(lines))


def body(gradient, prior_stat):
    experts = prior_stat.shape[0]
    slab_rows, width = gradient.shape[1:]
    blocks = slab_rows // ROWS
    columns = experts // blocks
    piece = width // columns
    pieces = gradient.reshape(blocks, ROWS, columns, piece).transpose(0, 2, 1, 3).reshape(experts, ROWS, piece)
    regrouped = exchanged(pieces, AXES)
    gram, lines = piece_gram(regrouped)
    gram_sum = summed_over_all(gram)
    statistic, scaled = grafted_products(slab_rows * width, gram_sum, prior_stat, lines)
    returned = exchanged(scaled, AXES)
    update = returned.reshape(blocks, columns, ROWS, piece).transpose(0, 2, 1, 3).reshape(gradient.shape)
    return (update, statistic)


def solution(mesh):
    torus = Mesh(
        mesh.devices.reshape(2, 2, 2, 2, 2, 2, 2, mesh.shape["layer"]),
        AXES + ("layer",),
    )
    return jax.shard_map(
        body,
        mesh=torus,
        in_specs=(P(LAYER_EXPERT, None, None), P("layer", None)),
        out_specs=(P(LAYER_EXPERT, None, None), P("layer", None)),
        check_vma=False,
    )
```

```python
import jax
import jax.numpy as jnp
from jax import lax
from jax.experimental import pallas as pl
from jax.experimental.pallas import tpu as pltpu
from jax.sharding import Mesh
from jax.sharding import PartitionSpec as P

ITERS = 5
AXES = ("z4", "z2", "z1", "y4", "y2", "y1", "core")
LAYER_EXPERT = ("layer",) + AXES
NEAR = ("z1", "y1", "core")
FAR = ("z4", "z2", "y4", "y2")

ridge_rate = 0.001
energy_floor = 1e-06

ROWS = 8
LANES = 128

VMEM = pl.BlockSpec(memory_space=pltpu.VMEM)


def matmul_high(left, right):
    return jnp.dot(left, right, precision=lax.Precision.HIGHEST, preferred_element_type=jnp.float32)


def split_three(wide):
    high = wide.astype(jnp.bfloat16)
    rest = wide - high.astype(jnp.float32)
    middle = rest.astype(jnp.bfloat16)
    return high, middle, (rest - middle.astype(jnp.float32)).astype(jnp.bfloat16)


def peers_of(axes):
    peers = 1
    for axis in axes:
        peers *= lax.axis_size(axis)
    return peers


def exchanged(pieces, axes):
    return lax.all_to_all(pieces, axes, split_axis=0, concat_axis=0, tiled=True)


def from_everyone(shard, axes):
    return exchanged(jnp.broadcast_to(shard[None], (peers_of(axes), *shard.shape)), axes)


def summed_over_all(gram):
    rows, width = gram.shape
    near = peers_of(NEAR)
    own = jnp.sum(exchanged(gram.reshape(near, rows // near, width), NEAR), axis=0)
    own = jnp.sum(from_everyone(own, FAR), axis=0)
    return from_everyone(own, NEAR).reshape(rows, width)


def in_vmem(array):
    return pltpu.with_memory_space_constraint(array, pltpu.VMEM)


def whole_sum(array):
    return jnp.sum(jnp.sum(array, axis=0, keepdims=True), axis=1, keepdims=True)


def widen_rows(pieces_ref, wide_ref):
    for tile in range(wide_ref.shape[0]):
        lanes = pieces_ref[:, :, tile * LANES : (tile + 1) * LANES]
        wide_ref[tile] = lanes.astype(jnp.float32).reshape(wide_ref.shape[1:])


def one_row(wide_ref, row, experts, rows):
    parts = [wide_ref[tile, pl.ds(row, experts, stride=rows), :] for tile in range(wide_ref.shape[0])]
    return jnp.concatenate(parts, axis=1).astype(jnp.bfloat16)


def wide_scratch(experts, rows, width):
    return pltpu.VMEM((width // LANES, experts * rows, LANES), jnp.float32)


def piece_gram(pieces):
    experts, rows, width = pieces.shape

    def kernel(pieces_ref, gram_ref, lines_ref, wide_ref):
        widen_rows(pieces_ref, wide_ref)
        gram = jnp.zeros((experts, experts), jnp.float32)
        for row in range(rows):
            line = one_row(wide_ref, row, experts, rows)
            lines_ref[row] = line
            gram += lax.dot_general(line, line, (((1,), (1,)), ((), ())), preferred_element_type=jnp.float32)
        gram_ref[...] = gram

    return pl.pallas_call(
        kernel,
        out_shape=(
            pltpu.VMEM((experts, experts), jnp.float32),
            pltpu.VMEM((rows, experts, width), jnp.bfloat16),
        ),
        in_specs=[VMEM],
        out_specs=(VMEM,) * 2,
        scratch_shapes=[wide_scratch(experts, rows, width)],
        name="piece_gram",
    )(in_vmem(pieces))


def grafted_products(entry_count, gram_sum, prior_stat, lines):
    rows, experts, width = lines.shape

    def kernel(gram_ref, prior_ref, lines_ref, stat_ref, update_ref, out_ref, held_ref, arrival):
        shape = (experts, experts)
        diagonal = lax.broadcasted_iota(jnp.int32, shape, 0) == lax.broadcasted_iota(jnp.int32, shape, 1)
        gram_mean = gram_ref[...] * (1.0 / entry_count)
        statistic = prior_ref[...] + gram_mean
        held_ref[...] = statistic
        written = pltpu.make_async_copy(held_ref, stat_ref, arrival)
        ridge = whole_sum(jnp.where(diagonal, statistic, 0.0)) * (ridge_rate / experts)
        shifted = statistic + jnp.where(diagonal, ridge, 0.0)
        start = 2.5 * lax.rsqrt(whole_sum(shifted * shifted))
        scaled_identity = jnp.where(diagonal, 1.25, 0.0)
        matrix = start * shifted
        factor = scaled_identity - 0.25 * matrix
        root = jnp.sqrt(jnp.sqrt(start)) * factor
        for repeat in range(ITERS - 1):
            square = matmul_high(factor, factor)
            matrix = matmul_high(matmul_high(square, square), matrix)
            factor = scaled_identity - 0.25 * matrix
            root = matmul_high(root, factor)
            if repeat == 0:
                written.start()
        root_bf = root.astype(jnp.bfloat16)
        root_gram = jnp.dot(
            jnp.concatenate([root_bf] * 3, axis=1),
            jnp.concatenate(split_three(gram_mean), axis=0),
            preferred_element_type=jnp.float32,
        )
        update_energy = whole_sum(root_gram * root_bf.astype(jnp.float32)) / experts
        grad_energy = whole_sum(jnp.where(diagonal, gram_mean, 0.0)) / experts
        graft = jnp.sqrt((grad_energy + energy_floor) / (update_energy + energy_floor))
        for row in range(0, rows, 2):
            pair = jnp.concatenate([lines_ref[row], lines_ref[row + 1]], axis=1)
            mixed_bf = jnp.dot(root_bf, pair, preferred_element_type=jnp.float32).astype(jnp.bfloat16)
            update = graft * mixed_bf.astype(jnp.float32)
            for part in range(2 * width // LANES):
                target = pl.ds(row + part * LANES // width, experts, stride=rows)
                out_ref[part % (width // LANES), target, :] = update[:, part * LANES : (part + 1) * LANES]
        for tile in range(width // LANES):
            update_ref[:, :, tile * LANES : (tile + 1) * LANES] = (
                out_ref[tile].reshape(experts, rows, LANES).astype(jnp.bfloat16)
            )
        written.wait()

    return pl.pallas_call(
        kernel,
        out_shape=(
            pltpu.HBM((experts, experts), jnp.float32),
            pltpu.VMEM((experts, rows, width), jnp.bfloat16),
        ),
        in_specs=[VMEM] * 3,
        out_specs=(pl.BlockSpec(memory_space=pltpu.HBM), VMEM),
        scratch_shapes=[
            wide_scratch(experts, rows, width),
            pltpu.VMEM((experts, experts), jnp.float32),
            pltpu.SemaphoreType.DMA,
        ],
        name="grafted_products",
    )(in_vmem(gram_sum), in_vmem(prior_stat), in_vmem(lines))


def body(gradient, prior_stat):
    experts = prior_stat.shape[0]
    slab_rows, width = gradient.shape[1:]
    blocks = slab_rows // ROWS
    columns = experts // blocks
    piece = width // columns
    pieces = gradient.reshape(blocks, ROWS, columns, piece).transpose(0, 2, 1, 3).reshape(experts, ROWS, piece)
    regrouped = exchanged(pieces, AXES)
    gram, lines = piece_gram(regrouped)
    gram_sum = summed_over_all(gram)
    statistic, scaled = grafted_products(slab_rows * width, gram_sum, prior_stat, lines)
    returned = exchanged(scaled, AXES)
    update = returned.reshape(blocks, columns, ROWS, piece).transpose(0, 2, 1, 3).reshape(gradient.shape)
    return (update, statistic)


def solution(mesh):
    torus = Mesh(
        mesh.devices.reshape(2, 2, 2, 2, 2, 2, 2, mesh.shape["layer"]),
        AXES + ("layer",),
    )
    return jax.shard_map(
        body,
        mesh=torus,
        in_specs=(P(LAYER_EXPERT, None, None), P("layer", None)),
        out_specs=(P(LAYER_EXPERT, None, None), P("layer", None)),
        check_vma=False,
    )
```
